32 devices in a mesh: rep: 2 (over x), dp: 16 (over y, z, core).
Axes of the slice: x: 2, y: 2, z: 4, core: 2. Of those that a mesh axis runs over, the one named last changes fastest.
Arguments:
- x: bfloat16 [32, 2048, 640], P(('rep', 'dp')), parts along dimension 0
- dy: bfloat16 [32, 2048, 640], P(('rep', 'dp')), parts along dimension 0
- wq: bfloat16 [2, 640, 640], P(None, 'dp')
- wk: bfloat16 [2, 640, 128], P(None, 'dp')
- wv: bfloat16 [2, 640, 128], P(None, 'dp')
- wo: bfloat16 [2, 640, 640], P(None, 'dp')
- w_gate: bfloat16 [2, 640, 2048], P(None, 'dp')
- w_up: bfloat16 [2, 640, 2048], P(None, 'dp')
- w_down: bfloat16 [2, 2048, 640], P(None, 'dp')
- m_wq: float32 [2, 640, 640], P(None, 'dp')
- m_wk: float32 [2, 640, 128], P(None, 'dp')
- m_wv: float32 [2, 640, 128], P(None, 'dp')
- m_wo: float32 [2, 640, 640], P(None, 'dp')
- m_w_gate: float32 [2, 640, 2048], P(None, 'dp')
- m_w_up: float32 [2, 640, 2048], P(None, 'dp')
- m_w_down: float32 [2, 2048, 640], P(None, 'dp')
- v_wq: float32 [2, 640, 640], P(None, 'dp')
- v_wk: float32 [2, 640, 128], P(None, 'dp')
- v_wv: float32 [2, 640, 128], P(None, 'dp')
- v_wo: float32 [2, 640, 640], P(None, 'dp')
- v_w_gate: float32 [2, 640, 2048], P(None, 'dp')
- v_w_up: float32 [2, 640, 2048], P(None, 'dp')
- v_w_down: float32 [2, 2048, 640], P(None, 'dp')
Outputs:
- output 1: bfloat16 [4, 640, 640], P('rep', 'dp'), parts along dimension 0
- output 2: bfloat16 [4, 640, 128], P('rep', 'dp'), parts along dimension 0
- output 3: bfloat16 [4, 640, 128], P('rep', 'dp'), parts along dimension 0
- output 4: bfloat16 [4, 640, 640], P('rep', 'dp'), parts along dimension 0
- output 5: bfloat16 [4, 640, 2048], P('rep', 'dp'), parts along dimension 0
- output 6: bfloat16 [4, 640, 2048], P('rep', 'dp'), parts along dimension 0
- output 7: bfloat16 [4, 2048, 640], P('rep', 'dp'), parts along dimension 0
- output 8: float32 [4, 640, 640], P('rep', 'dp'), parts along dimension 0
- output 9: float32 [4, 640, 128], P('rep', 'dp'), parts along dimension 0
- output 10: float32 [4, 640, 128], P('rep', 'dp'), parts along dimension 0
- output 11: float32 [4, 640, 640], P('rep', 'dp'), parts along dimension 0
- output 12: float32 [4, 640, 2048], P('rep', 'dp'), parts along dimension 0
- output 13: float32 [4, 640, 2048], P('rep', 'dp'), parts along dimension 0
- output 14: float32 [4, 2048, 640], P('rep', 'dp'), parts along dimension 0
- output 15: float32 [4, 640, 640], P('rep', 'dp'), parts along dimension 0
- output 16: float32 [4, 640, 128], P('rep', 'dp'), parts along dimension 0
- output 17: float32 [4, 640, 128], P('rep', 'dp'), parts along dimension 0
- output 18: float32 [4, 640, 640], P('rep', 'dp'), parts along dimension 0
- output 19: float32 [4, 640, 2048], P('rep', 'dp'), parts along dimension 0
- output 20: float32 [4, 640, 2048], P('rep', 'dp'), parts along dimension 0
- output 21: float32 [4, 2048, 640], P('rep', 'dp'), parts along dimension 0
There are 2 independent parts. The reference program is written for one: setup_inputs(seed, part) draws one part's arguments, and reference() takes and returns one part's arrays. A program takes and returns all parts, laid end to end along the dimension named above; an argument that names none is the same for every part.
All inputs are finite; a program needn't handle non-finite values.
Results may differ from the reference program's by a relative error of at most 0.0311.
Values are sent between devices in bfloat16 or wider.
A program may use at most 2 GiB of HBM per device.

```python
import jax
import jax.numpy as jnp
from jax import lax

SEQUENCES = 16
TOKENS = 2048
D = 640
HEADS = 5
KV_HEADS = 1
HEAD = 128
FF = 2048
LAYERS = 2
THETA = 10000
NAMES = ("wq", "wk", "wv", "wo", "w_gate", "w_up", "w_down")
SHAPES = {
    "wq": (LAYERS, D, HEADS * HEAD),
    "wk": (LAYERS, D, KV_HEADS * HEAD),
    "wv": (LAYERS, D, KV_HEADS * HEAD),
    "wo": (LAYERS, HEADS * HEAD, D),
    "w_gate": (LAYERS, D, FF),
    "w_up": (LAYERS, D, FF),
    "w_down": (LAYERS, FF, D),
}


def bump(key, n, height):
    away = (jnp.arange(n, dtype=jnp.int32) - jax.random.randint(key, (), 0, n, jnp.int32)) % n
    return jnp.where(away < n // 8, height, 1.0)


def together(key, own, strength):
    shared = jax.random.normal(key, own.shape[1:], jnp.float32)
    return (own + strength * shared) * lax.rsqrt(1 + strength * strength)


def setup_inputs(seed: int = 0, part: int = 0) -> dict:
    kx, kdy, ka, kb, kz, kf, kh, kl, *keys = jax.random.split(jax.random.key(seed), 8 + 3 * len(NAMES))
    kx, kdy, ka, kb = (jax.random.fold_in(k, part) for k in (kx, kdy, ka, kb))
    kw, km, kv = (keys[i::3] for i in range(3))
    shape = (SEQUENCES, TOKENS, D)
    much_x, much_dy = jax.random.uniform(kz, (2,), jnp.float32, 0.0, 1.0)
    loud = 2.0 ** jax.random.uniform(jax.random.fold_in(kz, 1), (), jnp.float32, -1.0, 2.0)
    layers = 2.0 ** jax.random.uniform(kl, (LAYERS, 1, 1), jnp.float32, -1.0, 1.0)
    times = {"wq": 1.0, "wk": 1.0, "wv": 2.0, "wo": layers, "w_gate": 1.0, "w_up": bump(kh, FF, 4.0), "w_down": layers}
    x = together(ka, jax.random.normal(kx, shape, jnp.float32), much_x) * bump(kf, D, 4.0)
    dy = together(kb, jax.random.normal(kdy, shape, jnp.float32), much_dy)
    drawn = {"x": x.astype(jnp.bfloat16), "dy": (loud * dy * (SEQUENCES * TOKENS) ** -0.5).astype(jnp.bfloat16)}
    for key, name in zip(kw, NAMES, strict=True):
        drawn[name] = (jax.random.normal(key, SHAPES[name], jnp.float32) * SHAPES[name][1] ** -0.5 * times[name]).astype(jnp.bfloat16)
    for key, name in zip(km, NAMES, strict=True):
        drawn[f"m_{name}"] = 0.1 * jax.random.normal(key, SHAPES[name], jnp.float32)
    for key, name in zip(kv, NAMES, strict=True):
        drawn[f"v_{name}"] = jax.random.uniform(key, SHAPES[name], jnp.float32, 0.02, 0.06)
    return drawn


def matmul(a, w):
    return jnp.dot(a, w, preferred_element_type=jnp.float32).astype(jnp.bfloat16)


def normed(h):
    wide = h.astype(jnp.float32)
    scale = lax.rsqrt(jnp.mean(wide**2, -1, keepdims=True) + 1e-6)
    return (wide * scale).astype(jnp.bfloat16)


def turned(t, theta):
    half = t.shape[-1] // 2
    angle = jnp.arange(t.shape[0], dtype=jnp.float32)[:, None] * theta ** (-jnp.arange(half, dtype=jnp.float32) / half)
    cos, sin = jnp.cos(angle)[:, None], jnp.sin(angle)[:, None]
    a, b = t[..., :half].astype(jnp.float32), t[..., half:].astype(jnp.float32)
    return jnp.concatenate([a * cos - b * sin, b * cos + a * sin], -1).astype(jnp.bfloat16)


def seen_by(q, k, v):
    tokens, kv = q.shape[0], k.shape[1]
    q = q.reshape(tokens, kv, -1, q.shape[-1])
    scores = jnp.einsum("tgsd,ugd->gstu", q.astype(jnp.float32), k.astype(jnp.float32)) * q.shape[-1] ** -0.5
    place = jnp.arange(tokens)
    weights = jax.nn.softmax(jnp.where(place[:, None] >= place, scores, -jnp.inf), -1).astype(jnp.bfloat16)
    return jnp.einsum("gstu,ugd->tgsd", weights.astype(jnp.float32), v.astype(jnp.float32)).astype(jnp.bfloat16).reshape(tokens, -1)


def layer(h, w):
    a = normed(h)
    q, k = (turned(matmul(a, w[name]).reshape(h.shape[0], -1, HEAD), THETA) for name in ("wq", "wk"))
    h = h + matmul(seen_by(q, k, matmul(a, w["wv"]).reshape(h.shape[0], -1, HEAD)), w["wo"])
    b = normed(h)
    gate = jnp.dot(b, w["w_gate"], preferred_element_type=jnp.float32)
    up = jnp.dot(b, w["w_up"], preferred_element_type=jnp.float32)
    return h + matmul((jax.nn.silu(gate) * up).astype(jnp.bfloat16), w["w_down"])


def adamw(w, m, v, g):
    m = 0.9 * m + 0.1 * g
    v = 0.95 * v + 0.05 * g * g
    step = m * lax.rsqrt(v + 1e-8) + 0.1 * w
    return (w - 0.02 * step).astype(jnp.bfloat16), m, v


def clipped(gradients, sum_of_squares, count):
    factor = jnp.minimum(1.0, 0.5 * lax.rsqrt(sum_of_squares / count + 1e-30))
    return [g * factor for g in gradients]


def stack(weights, h):
    return lax.scan(lambda h, w: (layer(h, w), None), h, weights)[0]


def reference(x, dy, wq, wk, wv, wo, w_gate, w_up, w_down, m_wq, m_wk, m_wv, m_wo, m_w_gate, m_w_up, m_w_down, v_wq, v_wk, v_wv, v_wo, v_w_gate, v_w_up, v_w_down):
    weights = dict(zip(NAMES, (wq, wk, wv, wo, w_gate, w_up, w_down), strict=True))

    def take(so_far, sequence):
        h, by_y = sequence
        _, back = jax.vjp(stack, weights, h)
        by_weights, by_h = back(by_y)
        return jax.tree.map(lambda total, term: total + term.astype(jnp.float32), so_far, by_weights), by_h

    none_yet = {name: jnp.zeros(w.shape, jnp.float32) for name, w in weights.items()}
    by_weights, by_x = lax.scan(take, none_yet, (x, dy))
    gradients = [by_weights[name].astype(jnp.bfloat16).astype(jnp.float32) for name in NAMES]
    gradients = clipped(gradients, sum(jnp.sum(g * g) for g in gradients), sum(g.size for g in gradients))
    first = (m_wq, m_wk, m_wv, m_wo, m_w_gate, m_w_up, m_w_down)
    second = (v_wq, v_wk, v_wv, v_wo, v_w_gate, v_w_up, v_w_down)
    new = [adamw(weights[name].astype(jnp.float32), m, v, g) for name, m, v, g in zip(NAMES, first, second, gradients, strict=True)]
    return tuple(one[which] for which in range(3) for one in new)
```

```python
import functools

import jax
import jax.numpy as jnp
from jax import lax
from jax.experimental import pallas as pl
from jax.experimental.pallas import tpu as pltpu

NEG = -1e30
LOG2E = 1.4426950408889634
VMEM = 56 * 2**20
HEADS = 5
HEAD = 128
BK = 512
LOW = jnp.bfloat16


def _dot(a, b, ca, cb):
    return lax.dot_general(a, b, (((ca,), (cb,)), ((), ())), preferred_element_type=jnp.float32)


def _spans(iq, bq):
    return lax.div(iq * bq, BK), lax.div(iq * bq + bq + BK - 1, BK)


def _gap(cols, bq):
    return lax.rem(lax.broadcasted_iota(jnp.int32, (BK, cols), 1), bq) - lax.broadcasted_iota(jnp.int32, (BK, cols), 0)


def _row(ref):
    return jnp.concatenate([ref[n : n + 1, :] for n in range(HEADS)], axis=1)


def _forward(q_ref, k_ref, v_ref, o_ref, lse_ref, top_s, mix_s, gap_s, *, scale, wide):
    bq = q_ref.shape[1]
    cols = HEADS * bq
    iq = pl.program_id(0)
    e = scale * LOG2E
    pieces = range(0, cols, wide)
    gap_s[...] = _gap(cols, bq)
    top_s[...] = jnp.full_like(top_s, NEG)
    mix_s[...] = jnp.zeros_like(mix_s)
    ones = jnp.ones((8, BK), LOW)

    def block(j, masked):
        here = pl.ds(j * BK, BK)
        scores = [_dot(k_ref[here, :], q_ref[...].reshape(cols, HEAD)[at : at + wide, :], 1, 1) for at in pieces]
        weights, keeps = [], []
        for at, s in zip(pieces, scores):
            if masked:
                s = jnp.where(gap_s[:, at : at + wide] >= j * BK - iq * bq, s, 2 * NEG)
            old = top_s[:, at : at + wide]
            top = jnp.maximum(old, s.max(axis=0, keepdims=True))
            top_s[:, at : at + wide] = top
            weights.append(jnp.exp2((s - top) * e).astype(LOW))
            keeps.append(jnp.exp2((old - top) * e))
        values = jnp.concatenate([v_ref[here, :].T, ones], axis=0)
        for at, p, keep in zip(pieces, weights, keeps):
            mix_s[:, at : at + wide] = mix_s[:, at : at + wide] * keep + _dot(values, p, 1, 0)

    whole, last = _spans(iq, bq)
    lax.fori_loop(0, whole, lambda j, _: block(j, False), None)
    lax.fori_loop(whole, last, lambda j, _: block(j, True), None)
    total = mix_s[HEAD : HEAD + 1, :]
    o_ref[...] = (mix_s[:HEAD, :] * (1 / total)).T.reshape(HEADS, bq, HEAD).astype(LOW)
    lse = top_s[...] * scale + jnp.log(total)
    for n in range(HEADS):
        lse_ref[n : n + 1, :] = lse[:, n * bq : (n + 1) * bq]


def _backward(q_ref, k_ref, v_ref, do_ref, lse_ref, delta_ref, dq_ref, dk_ref, dv_ref, dq_s, dk_s, dv_s, gap_s, *, scale, wide):
    bq = q_ref.shape[1]
    cols = HEADS * bq
    iq = pl.program_id(0)
    e = scale * LOG2E
    pieces = range(0, cols, wide)

    @pl.when(iq == 0)
    def _():
        gap_s[...] = _gap(cols, bq)
        dk_s[...] = jnp.zeros_like(dk_s)
        dv_s[...] = jnp.zeros_like(dv_s)

    dq_s[...] = jnp.zeros_like(dq_s)
    lses, deltas = _row(lse_ref) * LOG2E, _row(delta_ref)

    def block(j, masked):
        here = pl.ds(j * BK, BK)
        qs = [q_ref[...].reshape(cols, HEAD)[at : at + wide, :] for at in pieces]
        dos = [do_ref[...].reshape(cols, HEAD)[at : at + wide, :] for at in pieces]
        scores = [_dot(k_ref[here, :], x, 1, 1) for x in qs]
        dps = [_dot(v_ref[here, :], x, 1, 1) for x in dos]
        for n, at in enumerate(pieces):
            p = jnp.exp2(scores[n] * e - lses[:, at : at + wide])
            if masked:
                p = jnp.where(gap_s[:, at : at + wide] >= j * BK - iq * bq, p, 0.0)
            ds = (p * (dps[n] - deltas[:, at : at + wide])).astype(LOW)
            dv_s[here, :] += _dot(p.astype(LOW), dos[n], 1, 0)
            dk_s[here, :] += _dot(ds, qs[n], 1, 0)
            dq_s[:, at : at + wide] += _dot(k_ref[here, :].T, ds, 1, 0)

    whole, last = _spans(iq, bq)
    lax.fori_loop(0, whole, lambda j, _: block(j, False), None)
    lax.fori_loop(whole, last, lambda j, _: block(j, True), None)
    dq_ref[...] = (dq_s[...] * scale).T.reshape(HEADS, bq, HEAD).astype(LOW)

    @pl.when(iq == pl.num_programs(0) - 1)
    def _():
        dk_ref[...] = (dk_s[...] * scale).astype(LOW)
        dv_ref[...] = dv_s[...].astype(LOW)


def _attention_call(body, bq, wide, t, outs, scratch, dots, args):
    queries = pl.BlockSpec((HEADS, bq, HEAD), lambda i: (0, i, 0))
    keys = pl.BlockSpec((t, HEAD), lambda i: (0, 0))
    stats = pl.BlockSpec((HEADS, bq), lambda i: (0, i))
    kinds = {(HEADS, t, HEAD): queries, (t, HEAD): keys, (HEADS, t): stats}
    return pl.pallas_call(
        functools.partial(body, scale=HEAD**-0.5, wide=wide), grid=(t // bq,), in_specs=[kinds[a.shape] for a in args],
        out_specs=[kinds[a.shape] for a in outs], out_shape=outs, scratch_shapes=scratch,
        compiler_params=pltpu.CompilerParams(dimension_semantics=("arbitrary",), vmem_limit_bytes=VMEM),
        cost_estimate=pl.CostEstimate(flops=dots * HEADS * t * t * HEAD, transcendentals=HEADS * t * t,
                                      bytes_accessed=sum(a.size * a.dtype.itemsize for a in args)))(*args)


def attend(q, k, v, bq=512, wide=512):
    t, f32, cols = q.shape[1], jnp.float32, HEADS * bq
    return _attention_call(_forward, bq, wide, t, [jax.ShapeDtypeStruct(q.shape, LOW), jax.ShapeDtypeStruct((HEADS, t), f32)],
                           [pltpu.VMEM((1, cols), f32), pltpu.VMEM((HEAD + 8, cols), f32), pltpu.VMEM((BK, cols), jnp.int32)], 4, [q, k, v])


def attend_bwd(q, k, v, do, lse, delta, bq=256, wide=256):
    t, f32, cols = q.shape[1], jnp.float32, HEADS * bq
    return _attention_call(_backward, bq, wide, t, [jax.ShapeDtypeStruct(a.shape, LOW) for a in (q, k, v)],
                           [pltpu.VMEM((HEAD, cols), f32), pltpu.VMEM((t, HEAD), f32), pltpu.VMEM((t, HEAD), f32), pltpu.VMEM((BK, cols), jnp.int32)],
                           10, [q, k, v, do, lse, delta])


from jax.sharding import PartitionSpec as P

THETA = 10000
NAMES = ("wq", "wk", "wv", "wo", "w_gate", "w_up", "w_down")
BT = 512
CF = 512
ONCE = pl.Buffered(1)


def _rms(h):
    wide = h.astype(jnp.float32)
    scale = lax.rsqrt(jnp.mean(wide * wide, -1, keepdims=True) + 1e-6)
    return wide, scale


def _low(x):
    return x.astype(jnp.bfloat16)


def _wide(x):
    return x.astype(jnp.float32)


def _swap_tiles(src, dst):
    r = src.shape[0] // 16
    for m in range(8):
        for n in range(8):
            t = _wide(src[2 * r * m : 2 * r * (m + 1), 256 * n : 256 * (n + 1)])
            top = jnp.concatenate([t[:r, :128], t[r:, :128]], axis=1)
            low = jnp.concatenate([t[:r, 128:], t[r:, 128:]], axis=1)
            dst[2 * r * n : 2 * r * (n + 1), 256 * m : 256 * (m + 1)] = jnp.concatenate([top, low], axis=0).astype(dst.dtype)


def _project(h_ref, wa_ref, cos_ref, sin_ref, q_ref, k_ref, v_ref):
    wide, scale = _rms(h_ref[...])
    got = _wide(_low(_dot(_low(wide * scale), wa_ref[:, :896], 1, 0)))
    cos, sin = cos_ref[...], sin_ref[...]
    for i in range(6):
        t = got[:, 128 * i : 128 * (i + 1)]
        t = _low(t * cos + pltpu.roll(t, 64, 1) * sin)
        if i < 5:
            q_ref[i] = t
        else:
            k_ref[...] = t
    v_ref[...] = _low(got[:, 768:896])


def _heads(o_ref):
    return jnp.concatenate([o_ref[i] for i in range(o_ref.shape[0])], axis=1)


def _mlp(o_ref, h_ref, wg_ref, wu_ref, wd_ref, wa_ref, y_ref, wdt_s, b_s, sum_s):
    @pl.when(pl.program_id(0) == 0)
    def _():
        _swap_tiles(wd_ref, wdt_s)

    mid = _low(_wide(h_ref[...]) + _wide(_low(_dot(_heads(o_ref), wa_ref[:, 896:], 1, 0))))
    wide, scale = _rms(mid)
    b_s[...] = _low(wide * scale)
    sum_s[...] = jnp.zeros_like(sum_s)

    def chunk(c, _):
        at = pl.ds(pl.multiple_of(c * CF, CF), CF)
        gate, up = _dot(b_s[...], wg_ref[:, at], 1, 0), _dot(b_s[...], wu_ref[:, at], 1, 0)
        act = _low(gate * (1 / (1 + jnp.exp(-gate))) * up)
        sum_s[...] += _dot(act, wdt_s[:, at], 1, 1)

    lax.fori_loop(0, wg_ref.shape[1] // CF, chunk, None)
    y_ref[...] = _low(wide + _wide(_low(sum_s[...])))


def _mlp_back(*refs):
    o_ref, h_ref, dy_ref, wg_ref, wu_ref, wd_ref, wa_ref = refs[:7]
    dh_ref, do_ref, delta_ref, g_ref, dwo_ref = refs[7:12]
    wdt_s, ag_s, au_s, ad_s, ao_s, b_s, bt_s, dyt_s, db_s = refs[12:]
    step = pl.program_id(0)

    @pl.when(step == 0)
    def _():
        _swap_tiles(wd_ref, wdt_s)
        for s in (ag_s, au_s, ad_s, ao_s):
            s[...] = jnp.zeros_like(s)

    o = _heads(o_ref)
    mid = _low(_wide(h_ref[...]) + _wide(_low(_dot(o, wa_ref[:, 896:], 1, 0))))
    wide, scale = _rms(mid)
    b = _low(wide * scale)
    b_s[...] = b
    bt_s[...] = b.T
    dyt_s[...] = dy_ref[...].T
    db_s[...] = jnp.zeros_like(db_s)

    def chunk(c, _):
        at = pl.ds(pl.multiple_of(c * CF, CF), CF)
        gate, up = _dot(b_s[...], wg_ref[:, at], 1, 0), _dot(b_s[...], wu_ref[:, at], 1, 0)
        dact = _wide(_low(_dot(dy_ref[...], wdt_s[:, at], 1, 0)))
        s = 1 / (1 + jnp.exp(-gate))
        silu = gate * s
        act = _low(silu * up)
        dup = _low(dact * silu)
        dgate = _low(dact * up * (s + silu * (1 - s)))
        ad_s[:, at] += _dot(dyt_s[...], act, 1, 0)
        au_s[:, at] += _dot(bt_s[...], dup, 1, 0)
        ag_s[:, at] += _dot(bt_s[...], dgate, 1, 0)
        db_s[...] += _dot(dup, wu_ref[:, at], 1, 1) + _dot(dgate, wg_ref[:, at], 1, 1)

    lax.fori_loop(0, wg_ref.shape[1] // CF, chunk, None)
    db = _wide(_low(db_s[...]))
    wide, scale = _rms(_low(_wide(h_ref[...]) + _wide(_low(_dot(o, wa_ref[:, 896:], 1, 0)))))
    dn = scale * (db - wide * (scale * scale * jnp.mean(db * wide, -1, keepdims=True)))
    dh = _low(_wide(dy_ref[...]) + _wide(_low(dn)))
    dh_ref[...] = dh
    do = _low(_dot(dh, wa_ref[:, 896:], 1, 1))
    for i in range(5):
        part = do[:, 128 * i : 128 * (i + 1)]
        do_ref[i] = part
        delta_ref[i : i + 1, :] = (_wide(part) * _wide(o_ref[i])).T.sum(axis=0, keepdims=True)
    ao_s[...] += _dot(o.T, dh, 1, 0)

    @pl.when(step == pl.num_programs(0) - 1)
    def _():
        ff = wg_ref.shape[1]
        g_ref[:, :ff] = _low(ag_s[...])
        g_ref[:, ff : 2 * ff] = _low(au_s[...])
        _swap_tiles(ad_s, g_ref.at[:, 2 * ff : 3 * ff])
        dwo_ref[...] = _low(ao_s[...])


def _project_back(*refs, last):
    dq_ref, dk_ref, dv_ref, h_ref, cos_ref, sin_ref, dwo_ref, wa_ref = refs[:8]
    if last:
        g_ref, sum_s = refs[8:]
    else:
        dm_ref, dh_ref, g_ref, sum_s = refs[8:]
    step = pl.program_id(0)

    @pl.when(step == 0)
    def _():
        sum_s[...] = jnp.zeros_like(sum_s)

    cos, sin = cos_ref[...], sin_ref[...]
    parts = []
    for i in range(6):
        t = _wide(dq_ref[i] if i < 5 else dk_ref[...])
        parts.append(_low(t * cos - pltpu.roll(t, 64, 1) * sin))
    dqkv = jnp.concatenate(parts + [dv_ref[...]], axis=1)
    wide, scale = _rms(h_ref[...])
    sum_s[...] += _dot(_low(wide * scale).T, dqkv, 1, 0)
    if not last:
        da = _wide(_low(_dot(dqkv, wa_ref[:, :896], 1, 1)))
        dn = scale * (da - wide * (scale * scale * jnp.mean(da * wide, -1, keepdims=True)))
        dh_ref[...] = _low(_wide(dm_ref[...]) + _wide(_low(dn)))

    @pl.when(step == pl.num_programs(0) - 1)
    def _():
        g_ref[:, :896] = _low(sum_s[...])
        g_ref[:, 896:] = dwo_ref[...]


def _call(body, grid, ins, outs, scratch, flops, args, semantics="arbitrary"):
    size = sum(a.size * a.dtype.itemsize for a in args)
    return pl.pallas_call(
        body, grid=(grid,), in_specs=[s for s in ins], out_specs=[s for s, _ in outs], out_shape=[t for _, t in outs], scratch_shapes=scratch,
        compiler_params=pltpu.CompilerParams(dimension_semantics=(semantics,), vmem_limit_bytes=63 * 2**20),
        cost_estimate=pl.CostEstimate(flops=flops, transcendentals=0, bytes_accessed=size))(*args)


def _sizes(h):
    t, d = h.shape
    rows = pl.BlockSpec((BT, d), lambda i: (i, 0))
    heads = pl.BlockSpec((5, BT, HEAD), lambda i: (0, i, 0))
    head = pl.BlockSpec((BT, HEAD), lambda i: (i, 0))
    return t, d, rows, heads, head


def _part(d, ff, n, at):
    return pl.BlockSpec((d, 1536), lambda i: (0, 8 + at), pipeline_mode=ONCE) if n == 3 else pl.BlockSpec((d, ff), lambda i: (0, 3 * at + n), pipeline_mode=ONCE)


def _shape(s, t=jnp.bfloat16):
    return jax.ShapeDtypeStruct(s, t)


def project(h, slab, at, cos, sin):
    t, d, rows, heads, head = _sizes(h)
    return _call(_project, t // BT, [rows, _part(d, 2048, 3, at), head, head],
                 [(heads, _shape((5, t, HEAD))), (head, _shape((t, HEAD))), (head, _shape((t, HEAD)))], [],
                 2 * t * d * 896, [h, slab, cos, sin])


def mlp(o, h, slab, at):
    t, d, rows, heads, head = _sizes(h)
    ff = 2048
    return _call(_mlp, t // BT, [heads, rows] + [_part(d, ff, n, at) for n in range(4)], [(rows, _shape((t, d)))],
                 [pltpu.VMEM((d, ff), jnp.bfloat16), pltpu.VMEM((BT, d), jnp.bfloat16), pltpu.VMEM((BT, d), jnp.float32)],
                 2 * t * d * (d + 3 * ff), [o, h, slab, slab, slab, slab])[0]


def mlp_back(o, h, dy, slab, at):
    t, d, rows, heads, head = _sizes(h)
    ff = 2048
    whole = lambda s: pl.BlockSpec(s, lambda i: (0, 0), pipeline_mode=ONCE)
    wide = 3 * ff
    f32, b16 = jnp.float32, jnp.bfloat16
    return _call(_mlp_back, t // BT,
                 [heads, rows, rows] + [_part(d, ff, n, at) for n in range(4)],
                 [(rows, _shape((t, d))), (heads, _shape((5, t, HEAD))), (pl.BlockSpec((5, BT), lambda i: (0, i)), _shape((5, t), f32)),
                  (whole((d, wide)), _shape((d, wide))), (whole((d, d)), _shape((d, d)))],
                 [pltpu.VMEM((d, ff), b16), pltpu.VMEM((d, ff), f32), pltpu.VMEM((d, ff), f32), pltpu.VMEM((d, ff), f32), pltpu.VMEM((d, d), f32),
                  pltpu.VMEM((BT, d), b16), pltpu.VMEM((d, BT), b16), pltpu.VMEM((d, BT), b16), pltpu.VMEM((BT, d), f32)],
                 2 * t * d * (3 * d + 8 * ff), [o, h, dy, slab, slab, slab, slab])


def project_back(dq, dk, dv, h, cos, sin, dwo, slab, at, dm=None):
    t, d, rows, heads, head = _sizes(h)
    whole = lambda s: pl.BlockSpec(s, lambda i: (0, 0), pipeline_mode=ONCE)
    last = dm is None
    return _call(functools.partial(_project_back, last=last), t // BT,
                 [heads, head, head, rows, head, head, whole((d, d)), _part(d, 2048, 3, at)] + ([] if last else [rows]),
                 ([] if last else [(rows, _shape((t, d)))]) + [(whole((d, 1536)), _shape((d, 1536)))], [pltpu.VMEM((d, 896), jnp.float32)],
                 (2 if last else 4) * t * d * 896, [dq, dk, dv, h, cos, sin, dwo, slab] + ([] if last else [dm]))


def tables(t, theta):
    half = HEAD // 2
    angle = jnp.arange(t, dtype=jnp.float32)[:, None] * theta ** (-jnp.arange(half, dtype=jnp.float32) / half)
    cos, sin = jnp.cos(angle), jnp.sin(angle)
    return jnp.concatenate([cos, cos], 1), jnp.concatenate([-sin, sin], 1)


def adamw(w, m, v, g):
    m = 0.9 * m + 0.1 * g
    v = 0.95 * v + 0.05 * g * g
    step = m * lax.rsqrt(v + 1e-8) + 0.1 * w
    return (w - 0.02 * step).astype(jnp.bfloat16), m, v


def clipped(gradients, sum_of_squares, count):
    factor = jnp.minimum(1.0, 0.5 * lax.rsqrt(sum_of_squares / count + 1e-30))
    return [g * factor for g in gradients]


def laid(w):
    n, d = w["w_down"].shape
    down = w["w_down"].T.reshape(d * n // (128 * 40), 40, 128).transpose(1, 0, 2).reshape(40, -1)
    return [w["w_gate"], w["w_up"], down], [w["wq"], w["wk"], w["wv"], w["wo"]]


def parted(mlp, attn):
    ff = mlp.shape[1] // 3
    down = mlp[:, 2 * ff :].reshape(40, -1, 128).transpose(1, 0, 2).reshape(-1, 128).T
    return [attn[:, :640], attn[:, 640:768], attn[:, 768:896], attn[:, 896:], mlp[:, :ff], mlp[:, ff : 2 * ff], down]


def _total(n, x_ref, sum_ref, got, send, recv):
    me = lax.axis_index("dp")
    barrier = pltpu.get_barrier_semaphore()
    for k in range(1, n):
        pl.semaphore_signal(barrier, inc=1, device_id={"dp": lax.rem(me + k, n)}, device_id_type=pl.DeviceIdType.MESH)
    pl.semaphore_wait(barrier, n - 1)
    copies = [
        pltpu.make_async_remote_copy(src_ref=x_ref, dst_ref=got.at[me], send_sem=send.at[k - 1], recv_sem=recv.at[k - 1],
                                     device_id={"dp": lax.rem(me + k, n)}, device_id_type=pl.DeviceIdType.MESH)
        for k in range(1, n)
    ]
    for copy in copies:
        copy.start()
    got[me] = x_ref[...]
    for copy in copies:
        copy.wait()
    sum_ref[...] = functools.reduce(lambda a, b: a + b, [got[i] for i in range(n)])


def total(x, n):
    tile = (8, 128)
    vmem = pl.BlockSpec(memory_space=pltpu.VMEM)
    return pl.pallas_call(
        functools.partial(_total, n), out_shape=_shape(tile, jnp.float32), in_specs=[vmem], out_specs=vmem,
        scratch_shapes=[pltpu.VMEM((n, *tile), jnp.float32), pltpu.SemaphoreType.DMA((n - 1,)), pltpu.SemaphoreType.DMA((n - 1,))],
        compiler_params=pltpu.CompilerParams(collective_id=0, has_side_effects=True))(jnp.full(tile, x))[0, 0]


def solution(mesh):
    def scattered(g):
        return lax.psum_scatter(g, "dp", scatter_dimension=0, tiled=True)

    def step(x, dy, *arrays):
        weights, m, v = (arrays[i : i + 7] for i in (0, 7, 14))
        x, dy = x[0], dy[0]
        mlps, attns = zip(*(laid({name: w[n] for name, w in zip(NAMES, weights)}) for n in range(2)))
        slab = lax.all_gather(jnp.concatenate(sum(mlps + attns, []), 1), "dp", axis=0, tiled=True)
        cos, sin = tables(x.shape[0], THETA)

        hs, kept = [x], []
        for n in range(2):
            q, k, v_ = project(hs[n], slab, n, cos, sin)
            o, lse = attend(q, k, v_)
            kept.append((q, k, v_, o, lse))
            if n == 0:
                hs.append(mlp(o, x, slab, n))

        sums = [None, None]
        for n in (1, 0):
            q, k, v_, o, lse = kept[n]
            dm, do, delta, g, dwo = mlp_back(o, hs[n], dy, slab, n)
            back = (*attend_bwd(q, k, v_, do, lse, delta), hs[n], cos, sin, dwo, slab, n)
            *dy, more = project_back(*back, dm if n else None)
            g = jnp.concatenate([g, more], 1)
            if n:
                dy = dy[0]
            else:
                g, sums[1] = lax.optimization_barrier((g, sums[1]))
            sums[n] = scattered(g)

        both = [parted(s[:, :6144], s[:, 6144:]) for s in sums]
        gradients = [jnp.stack([both[n][i] for n in range(2)]).astype(jnp.float32) for i in range(7)]
        squares = total(sum(jnp.sum(_wide(s) ** 2) for s in sums), mesh.shape["dp"])
        gradients = clipped(gradients, squares, lax.psum(1, "dp") * sum(g.size for g in gradients))
        new = [adamw(w.astype(jnp.float32), m, v, g) for w, m, v, g in zip(weights, m, v, gradients, strict=True)]
        return tuple(one[which] for which in range(3) for one in new)

    states, cut = P(("rep", "dp"), None, None), P(None, "dp", None)
    return jax.shard_map(
        step,
        mesh=mesh,
        in_specs=(states, states) + (cut,) * 21,
        out_specs=(P("rep", "dp", None),) * 21,
        check_vma=False,
    )
```

```python
import functools

import jax
import jax.numpy as jnp
from jax import lax
from jax.experimental import pallas as pl
from jax.experimental.pallas import tpu as pltpu

NEG = -1e30
LOG2E = 1.4426950408889634
VMEM = 56 * 2**20
HEADS = 5
HEAD = 128
BK = 512
LOW = jnp.bfloat16


def _dot(a, b, ca, cb):
    return lax.dot_general(a, b, (((ca,), (cb,)), ((), ())), preferred_element_type=jnp.float32)


def _spans(iq, bq):
    return lax.div(iq * bq, BK), lax.div(iq * bq + bq + BK - 1, BK)


def _gap(cols, bq):
    return lax.rem(lax.broadcasted_iota(jnp.int32, (BK, cols), 1), bq) - lax.broadcasted_iota(jnp.int32, (BK, cols), 0)


def _row(ref):
    return jnp.concatenate([ref[n : n + 1, :] for n in range(HEADS)], axis=1)


def _forward(q_ref, k_ref, v_ref, o_ref, lse_ref, top_s, mix_s, gap_s, *, scale, wide):
    bq = q_ref.shape[1]
    cols = HEADS * bq
    iq = pl.program_id(0)
    e = scale * LOG2E
    pieces = range(0, cols, wide)
    gap_s[...] = _gap(cols, bq)
    top_s[...] = jnp.full_like(top_s, NEG)
    mix_s[...] = jnp.zeros_like(mix_s)
    ones = jnp.ones((8, BK), LOW)

    def block(j, masked):
        here = pl.ds(j * BK, BK)
        scores = [_dot(k_ref[here, :], q_ref[...].reshape(cols, HEAD)[at : at + wide, :], 1, 1) for at in pieces]
        weights, keeps = [], []
        for at, s in zip(pieces, scores):
            if masked:
                s = jnp.where(gap_s[:, at : at + wide] >= j * BK - iq * bq, s, 2 * NEG)
            old = top_s[:, at : at + wide]
            top = jnp.maximum(old, s.max(axis=0, keepdims=True))
            top_s[:, at : at + wide] = top
            weights.append(jnp.exp2((s - top) * e).astype(LOW))
            keeps.append(jnp.exp2((old - top) * e))
        values = jnp.concatenate([v_ref[here, :].T, ones], axis=0)
        for at, p, keep in zip(pieces, weights, keeps):
            mix_s[:, at : at + wide] = mix_s[:, at : at + wide] * keep + _dot(values, p, 1, 0)

    whole, last = _spans(iq, bq)
    lax.fori_loop(0, whole, lambda j, _: block(j, False), None)
    lax.fori_loop(whole, last, lambda j, _: block(j, True), None)
    total = mix_s[HEAD : HEAD + 1, :]
    o_ref[...] = (mix_s[:HEAD, :] * (1 / total)).T.reshape(HEADS, bq, HEAD).astype(LOW)
    lse = top_s[...] * scale + jnp.log(total)
    for n in range(HEADS):
        lse_ref[n : n + 1, :] = lse[:, n * bq : (n + 1) * bq]


def _backward(q_ref, k_ref, v_ref, do_ref, lse_ref, delta_ref, dq_ref, dk_ref, dv_ref, dq_s, dk_s, dv_s, gap_s, *, scale, wide):
    bq = q_ref.shape[1]
    cols = HEADS * bq
    iq = pl.program_id(0)
    e = scale * LOG2E
    pieces = range(0, cols, wide)

    @pl.when(iq == 0)
    def _():
        gap_s[...] = _gap(cols, bq)
        dk_s[...] = jnp.zeros_like(dk_s)
        dv_s[...] = jnp.zeros_like(dv_s)

    dq_s[...] = jnp.zeros_like(dq_s)
    lses, deltas = _row(lse_ref) * LOG2E, _row(delta_ref)

    def block(j, masked):
        here = pl.ds(j * BK, BK)
        qs = [q_ref[...].reshape(cols, HEAD)[at : at + wide, :] for at in pieces]
        dos = [do_ref[...].reshape(cols, HEAD)[at : at + wide, :] for at in pieces]
        scores = [_dot(k_ref[here, :], x, 1, 1) for x in qs]
        dps = [_dot(v_ref[here, :], x, 1, 1) for x in dos]
        for n, at in enumerate(pieces):
            p = jnp.exp2(scores[n] * e - lses[:, at : at + wide])
            if masked:
                p = jnp.where(gap_s[:, at : at + wide] >= j * BK - iq * bq, p, 0.0)
            ds = (p * (dps[n] - deltas[:, at : at + wide])).astype(LOW)
            dv_s[here, :] += _dot(p.astype(LOW), dos[n], 1, 0)
            dk_s[here, :] += _dot(ds, qs[n], 1, 0)
            dq_s[:, at : at + wide] += _dot(k_ref[here, :].T, ds, 1, 0)

    whole, last = _spans(iq, bq)
    lax.fori_loop(0, whole, lambda j, _: block(j, False), None)
    lax.fori_loop(whole, last, lambda j, _: block(j, True), None)
    dq_ref[...] = (dq_s[...] * scale).T.reshape(HEADS, bq, HEAD).astype(LOW)

    @pl.when(iq == pl.num_programs(0) - 1)
    def _():
        dk_ref[...] = (dk_s[...] * scale).astype(LOW)
        dv_ref[...] = dv_s[...].astype(LOW)


def _attention_call(body, bq, wide, t, outs, scratch, dots, args):
    queries = pl.BlockSpec((HEADS, bq, HEAD), lambda i: (0, i, 0))
    keys = pl.BlockSpec((t, HEAD), lambda i: (0, 0))
    stats = pl.BlockSpec((HEADS, bq), lambda i: (0, i))
    kinds = {(HEADS, t, HEAD): queries, (t, HEAD): keys, (HEADS, t): stats}
    return pl.pallas_call(
        functools.partial(body, scale=HEAD**-0.5, wide=wide), grid=(t // bq,), in_specs=[kinds[a.shape] for a in args],
        out_specs=[kinds[a.shape] for a in outs], out_shape=outs, scratch_shapes=scratch,
        compiler_params=pltpu.CompilerParams(dimension_semantics=("arbitrary",), vmem_limit_bytes=VMEM),
        cost_estimate=pl.CostEstimate(flops=dots * HEADS * t * t * HEAD, transcendentals=HEADS * t * t,
                                      bytes_accessed=sum(a.size * a.dtype.itemsize for a in args)))(*args)


def attend(q, k, v, bq=512, wide=512):
    t, f32, cols = q.shape[1], jnp.float32, HEADS * bq
    return _attention_call(_forward, bq, wide, t, [jax.ShapeDtypeStruct(q.shape, LOW), jax.ShapeDtypeStruct((HEADS, t), f32)],
                           [pltpu.VMEM((1, cols), f32), pltpu.VMEM((HEAD + 8, cols), f32), pltpu.VMEM((BK, cols), jnp.int32)], 4, [q, k, v])


def attend_bwd(q, k, v, do, lse, delta, bq=256, wide=256):
    t, f32, cols = q.shape[1], jnp.float32, HEADS * bq
    return _attention_call(_backward, bq, wide, t, [jax.ShapeDtypeStruct(a.shape, LOW) for a in (q, k, v)],
                           [pltpu.VMEM((HEAD, cols), f32), pltpu.VMEM((t, HEAD), f32), pltpu.VMEM((t, HEAD), f32), pltpu.VMEM((BK, cols), jnp.int32)],
                           10, [q, k, v, do, lse, delta])


from jax.sharding import PartitionSpec as P

THETA = 10000
NAMES = ("wq", "wk", "wv", "wo", "w_gate", "w_up", "w_down")
BT = 512
CF = 512
ONCE = pl.Buffered(1)


def _rms(h):
    wide = h.astype(jnp.float32)
    scale = lax.rsqrt(jnp.mean(wide * wide, -1, keepdims=True) + 1e-6)
    return wide, scale


def _low(x):
    return x.astype(jnp.bfloat16)


def _wide(x):
    return x.astype(jnp.float32)


def _swap_tiles(src, dst):
    r = src.shape[0] // 16
    for m in range(8):
        for n in range(8):
            t = _wide(src[2 * r * m : 2 * r * (m + 1), 256 * n : 256 * (n + 1)])
            top = jnp.concatenate([t[:r, :128], t[r:, :128]], axis=1)
            low = jnp.concatenate([t[:r, 128:], t[r:, 128:]], axis=1)
            dst[2 * r * n : 2 * r * (n + 1), 256 * m : 256 * (m + 1)] = jnp.concatenate([top, low], axis=0).astype(dst.dtype)


def _project(h_ref, cos_ref, sin_ref, *refs):
    *w_refs, q_ref, k_ref, v_ref = refs
    wide, scale = _rms(h_ref[...])
    a = _low(wide * scale)
    got = jnp.concatenate([_wide(_low(_dot(a, w[...], 1, 0))) for w in w_refs], axis=1)
    cos, sin = cos_ref[...], sin_ref[...]
    for i in range(6):
        t = got[:, 128 * i : 128 * (i + 1)]
        t = _low(t * cos + pltpu.roll(t, 64, 1) * sin)
        if i < 5:
            q_ref[i] = t
        else:
            k_ref[...] = t
    v_ref[...] = _low(got[:, 768:896])


def _out(wa_ref):
    return wa_ref[:, wa_ref.shape[1] - HEADS * HEAD :]


def _heads(o_ref):
    return jnp.concatenate([o_ref[i] for i in range(o_ref.shape[0])], axis=1)


def _mlp(o_ref, h_ref, wg_ref, wu_ref, wd_ref, wa_ref, y_ref, wdt_s, b_s, sum_s):
    @pl.when(pl.program_id(0) == 0)
    def _():
        _swap_tiles(wd_ref, wdt_s)

    mid = _low(_wide(h_ref[...]) + _wide(_low(_dot(_heads(o_ref), _out(wa_ref), 1, 0))))
    wide, scale = _rms(mid)
    b_s[...] = _low(wide * scale)
    sum_s[...] = jnp.zeros_like(sum_s)

    def chunk(c, _):
        at = pl.ds(pl.multiple_of(c * 2 * CF, 2 * CF), 2 * CF)
        gate, up = _dot(b_s[...], wg_ref[:, at], 1, 0), _dot(b_s[...], wu_ref[:, at], 1, 0)
        act = _low(gate * (1 / (1 + jnp.exp(-gate))) * up)
        sum_s[...] += _dot(act, wdt_s[:, at], 1, 1)

    lax.fori_loop(0, wg_ref.shape[1] // (2 * CF), chunk, None)
    y_ref[...] = _low(wide + _wide(_low(sum_s[...])))


def _mlp_back(*refs, joined):
    o_ref, h_ref, dy_ref, wg_ref, wu_ref, wd_ref, wa_ref = refs[:7]
    dh_ref, do_ref, delta_ref, g_ref, dwo_ref = refs[7 + joined : 12 + joined]
    wdt_s, ag_s, au_s, ad_s, ao_s, b_s, bt_s, dyt_s, db_s = refs[12 + joined :]
    step = pl.program_id(0)

    @pl.when(step == 0)
    def _():
        _swap_tiles(wd_ref, wdt_s)
        for s in (ag_s, au_s, ad_s, ao_s):
            s[...] = jnp.zeros_like(s)

    o = _heads(o_ref)
    mid = _low(_wide(h_ref[...]) + _wide(_low(_dot(o, _out(wa_ref), 1, 0))))
    wide, scale = _rms(mid)
    b = _low(wide * scale)
    b_s[...] = b
    bt_s[...] = b.T
    dyt_s[...] = dy_ref[...].T
    db_s[...] = jnp.zeros_like(db_s)

    def chunk(c):
        at = pl.ds(c * CF, CF)
        gate, up = _dot(b_s[...], wg_ref[:, at], 1, 0), _dot(b_s[...], wu_ref[:, at], 1, 0)
        dact = _wide(_low(_dot(dy_ref[...], wdt_s[:, at], 1, 0)))
        s = 1 / (1 + jnp.exp(-gate))
        silu = gate * s
        act = _low(silu * up)
        dup = _low(dact * silu)
        dgate = _low(dact * up * (s + silu * (1 - s)))
        ad_s[:, at] += _dot(dyt_s[...], act, 1, 0)
        au_s[:, at] += _dot(bt_s[...], dup, 1, 0)
        ag_s[:, at] += _dot(bt_s[...], dgate, 1, 0)
        db_s[...] += _dot(dup, wu_ref[:, at], 1, 1) + _dot(dgate, wg_ref[:, at], 1, 1)

    for c in range(wg_ref.shape[1] // CF):
        chunk(c)
    db = _wide(_low(db_s[...]))
    wide, scale = _rms(_low(_wide(h_ref[...]) + _wide(_low(_dot(o, _out(wa_ref), 1, 0)))))
    dn = scale * (db - wide * (scale * scale * jnp.mean(db * wide, -1, keepdims=True)))
    dh = _low(_wide(dy_ref[...]) + _wide(_low(dn)))
    dh_ref[...] = dh
    do = _low(_dot(dh, _out(wa_ref), 1, 1))
    for i in range(5):
        part = do[:, 128 * i : 128 * (i + 1)]
        do_ref[i] = part
        delta_ref[i : i + 1, :] = (_wide(part) * _wide(o_ref[i])).T.sum(axis=0, keepdims=True)
    ao_s[...] += _dot(o.T, dh, 1, 0)

    @pl.when(step == pl.num_programs(0) - 1)
    def _():
        ff = wg_ref.shape[1]
        g_ref[:, :ff] = _low(ag_s[...])
        g_ref[:, ff : 2 * ff] = _low(au_s[...])
        _swap_tiles(ad_s, g_ref.at[:, 2 * ff : 3 * ff])
        if joined:
            g_ref[:, 3 * ff :] = refs[7][...]
        dwo_ref[...] = _low(ao_s[...])


def _project_back(*refs, last):
    dq_ref, dk_ref, dv_ref, h_ref, cos_ref, sin_ref, dwo_ref = refs[:7]
    if last:
        g_ref, sum_s = refs[7:]
    else:
        wa_ref, dm_ref, dh_ref, g_ref, sum_s = refs[7:]
    step = pl.program_id(0)

    @pl.when(step == 0)
    def _():
        sum_s[...] = jnp.zeros_like(sum_s)

    cos, sin = cos_ref[...], sin_ref[...]
    parts = []
    for i in range(6):
        t = _wide(dq_ref[i] if i < 5 else dk_ref[...])
        parts.append(_low(t * cos - pltpu.roll(t, 64, 1) * sin))
    dqkv = jnp.concatenate(parts + [dv_ref[...]], axis=1)
    wide, scale = _rms(h_ref[...])
    sum_s[...] += _dot(_low(wide * scale).T, dqkv, 1, 0)
    if not last:
        da = _wide(_low(_dot(dqkv, wa_ref[:, :896], 1, 1)))
        dn = scale * (da - wide * (scale * scale * jnp.mean(da * wide, -1, keepdims=True)))
        dh_ref[...] = _low(_wide(dm_ref[...]) + _wide(_low(dn)))

    @pl.when(step == pl.num_programs(0) - 1)
    def _():
        g_ref[:, :896] = _low(sum_s[...])
        g_ref[:, 896:] = dwo_ref[...]


def _call(body, grid, ins, outs, scratch, flops, args, semantics="arbitrary"):
    size = sum(a.size * a.dtype.itemsize for a in args)
    return pl.pallas_call(
        body, grid=(grid,), in_specs=[s for s in ins], out_specs=[s for s, _ in outs], out_shape=[t for _, t in outs], scratch_shapes=scratch,
        compiler_params=pltpu.CompilerParams(dimension_semantics=(semantics,), vmem_limit_bytes=63 * 2**20),
        cost_estimate=pl.CostEstimate(flops=flops, transcendentals=0, bytes_accessed=size))(*args)


def _sizes(h):
    t, d = h.shape
    rows = pl.BlockSpec((BT, d), lambda i: (i, 0))
    heads = pl.BlockSpec((5, BT, HEAD), lambda i: (0, i, 0))
    head = pl.BlockSpec((BT, HEAD), lambda i: (i, 0))
    return t, d, rows, heads, head


def _part(d, ff, n, at):
    if n == 3:
        return pl.BlockSpec((d, 1536), lambda i: (0, 8), pipeline_mode=ONCE) if at else pl.BlockSpec((d, d), lambda i: (0, 22), pipeline_mode=ONCE)
    return pl.BlockSpec((d, ff), lambda i: (0, 3 * at + n), pipeline_mode=ONCE)


def _shape(s, t=jnp.bfloat16):
    return jax.ShapeDtypeStruct(s, t)


def project(h, cos, sin, *ws):
    t, d, rows, heads, head = _sizes(h)
    return _call(_project, t // BT, [rows, head, head] + [pl.BlockSpec((d, w.shape[1]), lambda i: (0, 0), pipeline_mode=ONCE) for w in ws],
                 [(heads, _shape((5, t, HEAD))), (head, _shape((t, HEAD))), (head, _shape((t, HEAD)))], [],
                 2 * t * d * 896, [h, cos, sin, *ws])


def mlp(o, h, slab, at):
    t, d, rows, heads, head = _sizes(h)
    ff = 2048
    return _call(_mlp, t // BT, [heads, rows] + [_part(d, ff, n, at) for n in range(4)], [(rows, _shape((t, d)))],
                 [pltpu.VMEM((d, ff), jnp.bfloat16), pltpu.VMEM((BT, d), jnp.bfloat16), pltpu.VMEM((BT, d), jnp.float32)],
                 2 * t * d * (d + 3 * ff), [o, h, slab, slab, slab, slab])[0]


def mlp_back(o, h, dy, slab, at, more=()):
    t, d, rows, heads, head = _sizes(h)
    ff = 2048
    whole = lambda s: pl.BlockSpec(s, lambda i: (0, 0), pipeline_mode=ONCE)
    wide = 3 * ff + sum(a.shape[1] for a in more)
    f32, b16 = jnp.float32, jnp.bfloat16
    return _call(functools.partial(_mlp_back, joined=len(more)), t // BT,
                 [heads, rows, rows] + [_part(d, ff, n, at) for n in range(4)] + [whole(a.shape) for a in more],
                 [(rows, _shape((t, d))), (heads, _shape((5, t, HEAD))), (pl.BlockSpec((5, BT), lambda i: (0, i)), _shape((5, t), f32)),
                  (whole((d, wide)), _shape((d, wide))), (whole((d, d)), _shape((d, d)))],
                 [pltpu.VMEM((d, ff), b16), pltpu.VMEM((d, ff), f32), pltpu.VMEM((d, ff), f32), pltpu.VMEM((d, ff), f32), pltpu.VMEM((d, d), f32),
                  pltpu.VMEM((BT, d), b16), pltpu.VMEM((d, BT), b16), pltpu.VMEM((d, BT), b16), pltpu.VMEM((BT, d), f32)],
                 2 * t * d * (3 * d + 8 * ff), [o, h, dy, slab, slab, slab, slab, *more])


def project_back(dq, dk, dv, h, cos, sin, dwo, slab=None, dm=None):
    t, d, rows, heads, head = _sizes(h)
    whole = lambda s: pl.BlockSpec(s, lambda i: (0, 0), pipeline_mode=ONCE)
    last = dm is None
    return _call(functools.partial(_project_back, last=last), t // BT,
                 [heads, head, head, rows, head, head, whole((d, d))] + ([] if last else [_part(d, 2048, 3, 1), rows]),
                 ([] if last else [(rows, _shape((t, d)))]) + [(whole((d, 1536)), _shape((d, 1536)))], [pltpu.VMEM((d, 896), jnp.float32)],
                 (2 if last else 4) * t * d * 896, [dq, dk, dv, h, cos, sin, dwo] + ([] if last else [slab, dm]))


def tables(t, theta):
    half = HEAD // 2
    angle = jnp.arange(t, dtype=jnp.float32)[:, None] * theta ** (-jnp.arange(half, dtype=jnp.float32) / half)
    cos, sin = jnp.cos(angle), jnp.sin(angle)
    return jnp.concatenate([cos, cos], 1), jnp.concatenate([-sin, sin], 1)


def adamw(w, m, v, g):
    m = 0.9 * m + 0.1 * g
    v = 0.95 * v + 0.05 * g * g
    step = m * lax.rsqrt(v + 1e-8) + 0.1 * w
    return (w - 0.02 * step).astype(jnp.bfloat16), m, v


def clipped(gradients, sum_of_squares, count):
    factor = jnp.minimum(1.0, 0.5 * lax.rsqrt(sum_of_squares / count + 1e-30))
    return [g * factor for g in gradients]


def laid(w):
    n, d = w["w_down"].shape
    down = w["w_down"].T.reshape(d * n // (128 * 40), 40, 128).transpose(1, 0, 2).reshape(40, -1)
    return [w["w_gate"], w["w_up"], down], [w["wq"], w["wk"], w["wv"], w["wo"]]


def parted(mlp, attn):
    ff = mlp.shape[1] // 3
    down = mlp[:, 2 * ff :].reshape(40, -1, 128).transpose(1, 0, 2).reshape(-1, 128).T
    return [attn[:, :640], attn[:, 640:768], attn[:, 768:896], attn[:, 896:], mlp[:, :ff], mlp[:, ff : 2 * ff], down]


def _total(n, x_ref, sum_ref, got, send, recv):
    me = lax.axis_index("dp")
    barrier = pltpu.get_barrier_semaphore()
    for k in range(1, n):
        pl.semaphore_signal(barrier, inc=1, device_id={"dp": lax.rem(me + k, n)}, device_id_type=pl.DeviceIdType.MESH)
    pl.semaphore_wait(barrier, n - 1)
    copies = [
        pltpu.make_async_remote_copy(src_ref=x_ref, dst_ref=got.at[me], send_sem=send.at[k - 1], recv_sem=recv.at[k - 1],
                                     device_id={"dp": lax.rem(me + k, n)}, device_id_type=pl.DeviceIdType.MESH)
        for k in range(1, n)
    ]
    for copy in copies:
        copy.start()
    got[me] = x_ref[...]
    for copy in copies:
        copy.wait()
    sum_ref[...] = functools.reduce(lambda a, b: a + b, [got[i] for i in range(n)])


def total(x, n):
    tile = (8, 128)
    vmem = pl.BlockSpec(memory_space=pltpu.VMEM)
    return pl.pallas_call(
        functools.partial(_total, n), out_shape=_shape(tile, jnp.float32), in_specs=[vmem], out_specs=vmem,
        scratch_shapes=[pltpu.VMEM((n, *tile), jnp.float32), pltpu.SemaphoreType.DMA((n - 1,)), pltpu.SemaphoreType.DMA((n - 1,))],
        compiler_params=pltpu.CompilerParams(collective_id=0, has_side_effects=True))(jnp.full(tile, x))[0, 0]


def solution(mesh):
    def scattered(g):
        return lax.psum_scatter(g, "dp", scatter_dimension=0, tiled=True)

    def step(x, dy, *arrays):
        weights, m, v = (arrays[i : i + 7] for i in (0, 7, 14))
        x, dy = x[0], dy[0]
        def gathered(*parts):
            return lax.all_gather(jnp.concatenate(parts, 1), "dp", axis=0, tiled=True)

        mlps, attns = zip(*(laid({name: w[n] for name, w in zip(NAMES, weights)}) for n in range(2)))
        wq, wkv = gathered(attns[0][0]), gathered(*attns[0][1:3])
        slab = gathered(*mlps[0], *mlps[1], *attns[1], *attns[0][1:])
        cos, sin = tables(x.shape[0], THETA)

        q, k, v_ = project(x, cos, sin, wq, wkv)
        o, lse = attend(q, k, v_)
        h = mlp(o, x, slab, 0)
        kept = q, k, v_, o, lse
        q, k, v_ = project(h, cos, sin, slab[:, 12288:13184])
        o, lse = attend(q, k, v_)

        dm, do, delta, g, dwo = mlp_back(o, h, dy, slab, 1)
        first = scattered(g)
        dy, more = project_back(*attend_bwd(q, k, v_, do, lse, delta), h, cos, sin, dwo, slab, dm)
        q, k, v_, o, lse = kept
        dm, do, delta, g, dwo = mlp_back(o, x, dy, slab, 0, [more])
        g, first = lax.optimization_barrier((g, first))
        second = scattered(g)
        g = project_back(*attend_bwd(q, k, v_, do, lse, delta), x, cos, sin, dwo)[0]
        terms = lax.all_to_all(g.reshape(-1, 40, g.shape[1]), "dp", 0, 0, tiled=True)
        third = lax.reduce_precision(_wide(terms).sum(0), 8, 7)
        sums = first, second, third

        both = [parted(second[:, :6144], third), parted(first, second[:, 6144:])]
        gradients = [jnp.stack([both[n][i] for n in range(2)]).astype(jnp.float32) for i in range(7)]
        squares = total(sum(jnp.sum(_wide(s) ** 2) for s in sums), mesh.shape["dp"])
        gradients = clipped(gradients, squares, lax.psum(1, "dp") * sum(g.size for g in gradients))
        new = [adamw(w.astype(jnp.float32), m, v, g) for w, m, v, g in zip(weights, m, v, gradients, strict=True)]
        return tuple(one[which] for which in range(3) for one in new)

    states, cut = P(("rep", "dp"), None, None), P(None, "dp", None)
    return jax.shard_map(
        step,
        mesh=mesh,
        in_specs=(states, states) + (cut,) * 21,
        out_specs=(P("rep", "dp", None),) * 21,
        check_vma=False,
    )
```

```python
import functools

import jax
import jax.numpy as jnp
from jax import lax
from jax.experimental import pallas as pl
from jax.experimental.pallas import tpu as pltpu

NEG = -1e30
LOG2E = 1.4426950408889634
VMEM = 56 * 2**20
HEADS = 5
HEAD = 128
BK = 512
LOW = jnp.bfloat16


def _dot(a, b, ca, cb):
    return lax.dot_general(a, b, (((ca,), (cb,)), ((), ())), preferred_element_type=jnp.float32)


def _spans(iq, bq):
    return lax.div(iq * bq, BK), lax.div(iq * bq + bq + BK - 1, BK)


def _gap(cols, bq):
    return lax.rem(lax.broadcasted_iota(jnp.int32, (BK, cols), 1), bq) - lax.broadcasted_iota(jnp.int32, (BK, cols), 0)


def _row(ref):
    return jnp.concatenate([ref[n : n + 1, :] for n in range(HEADS)], axis=1)


def _forward(q_ref, k_ref, v_ref, o_ref, lse_ref, top_s, mix_s, gap_s, *, scale, wide):
    bq = q_ref.shape[1]
    cols = HEADS * bq
    iq = pl.program_id(0)
    e = scale * LOG2E
    pieces = range(0, cols, wide)
    gap_s[...] = _gap(cols, bq)
    top_s[...] = jnp.full_like(top_s, NEG)
    mix_s[...] = jnp.zeros_like(mix_s)
    ones = jnp.ones((8, BK), LOW)

    def block(j, masked):
        here = pl.ds(j * BK, BK)
        scores = [_dot(k_ref[here, :], q_ref[...].reshape(cols, HEAD)[at : at + wide, :], 1, 1) for at in pieces]
        weights, keeps = [], []
        for at, s in zip(pieces, scores):
            if masked:
                s = jnp.where(gap_s[:, at : at + wide] >= j * BK - iq * bq, s, 2 * NEG)
            old = top_s[:, at : at + wide]
            top = jnp.maximum(old, s.max(axis=0, keepdims=True))
            top_s[:, at : at + wide] = top
            weights.append(jnp.exp2((s - top) * e).astype(LOW))
            keeps.append(jnp.exp2((old - top) * e))
        values = jnp.concatenate([v_ref[here, :].T, ones], axis=0)
        for at, p, keep in zip(pieces, weights, keeps):
            mix_s[:, at : at + wide] = mix_s[:, at : at + wide] * keep + _dot(values, p, 1, 0)

    whole, last = _spans(iq, bq)
    lax.fori_loop(0, whole, lambda j, _: block(j, False), None)
    lax.fori_loop(whole, last, lambda j, _: block(j, True), None)
    total = mix_s[HEAD : HEAD + 1, :]
    o_ref[...] = (mix_s[:HEAD, :] * (1 / total)).T.reshape(HEADS, bq, HEAD).astype(LOW)
    lse = top_s[...] * scale + jnp.log(total)
    for n in range(HEADS):
        lse_ref[n : n + 1, :] = lse[:, n * bq : (n + 1) * bq]


def _backward(q_ref, k_ref, v_ref, do_ref, lse_ref, delta_ref, dq_ref, dk_ref, dv_ref, dq_s, dk_s, dv_s, gap_s, *, scale, wide):
    bq = q_ref.shape[1]
    cols = HEADS * bq
    iq = pl.program_id(0)
    e = scale * LOG2E
    pieces = range(0, cols, wide)

    @pl.when(iq == 0)
    def _():
        gap_s[...] = _gap(cols, bq)
        dk_s[...] = jnp.zeros_like(dk_s)
        dv_s[...] = jnp.zeros_like(dv_s)

    dq_s[...] = jnp.zeros_like(dq_s)
    lses, deltas = _row(lse_ref) * LOG2E, _row(delta_ref)

    def block(j, masked):
        here = pl.ds(j * BK, BK)
        qs = [q_ref[...].reshape(cols, HEAD)[at : at + wide, :] for at in pieces]
        dos = [do_ref[...].reshape(cols, HEAD)[at : at + wide, :] for at in pieces]
        scores = [_dot(k_ref[here, :], x, 1, 1) for x in qs]
        dps = [_dot(v_ref[here, :], x, 1, 1) for x in dos]
        for n, at in enumerate(pieces):
            p = jnp.exp2(scores[n] * e - lses[:, at : at + wide])
            if masked:
                p = jnp.where(gap_s[:, at : at + wide] >= j * BK - iq * bq, p, 0.0)
            ds = (p * (dps[n] - deltas[:, at : at + wide])).astype(LOW)
            dv_s[here, :] += _dot(p.astype(LOW), dos[n], 1, 0)
            dk_s[here, :] += _dot(ds, qs[n], 1, 0)
            dq_s[:, at : at + wide] += _dot(k_ref[here, :].T, ds, 1, 0)

    whole, last = _spans(iq, bq)
    lax.fori_loop(0, whole, lambda j, _: block(j, False), None)
    lax.fori_loop(whole, last, lambda j, _: block(j, True), None)
    dq_ref[...] = (dq_s[...] * scale).T.reshape(HEADS, bq, HEAD).astype(LOW)

    @pl.when(iq == pl.num_programs(0) - 1)
    def _():
        dk_ref[...] = (dk_s[...] * scale).astype(LOW)
        dv_ref[...] = dv_s[...].astype(LOW)


def _attention_call(body, bq, wide, t, outs, scratch, dots, args):
    queries = pl.BlockSpec((HEADS, bq, HEAD), lambda i: (0, i, 0))
    keys = pl.BlockSpec((t, HEAD), lambda i: (0, 0))
    stats = pl.BlockSpec((HEADS, bq), lambda i: (0, i))
    kinds = {(HEADS, t, HEAD): queries, (t, HEAD): keys, (HEADS, t): stats}
    return pl.pallas_call(
        functools.partial(body, scale=HEAD**-0.5, wide=wide), grid=(t // bq,), in_specs=[kinds[a.shape] for a in args],
        out_specs=[kinds[a.shape] for a in outs], out_shape=outs, scratch_shapes=scratch,
        compiler_params=pltpu.CompilerParams(dimension_semantics=("arbitrary",), vmem_limit_bytes=VMEM),
        cost_estimate=pl.CostEstimate(flops=dots * HEADS * t * t * HEAD, transcendentals=HEADS * t * t,
                                      bytes_accessed=sum(a.size * a.dtype.itemsize for a in args)))(*args)


def attend(q, k, v, bq=512, wide=512):
    t, f32, cols = q.shape[1], jnp.float32, HEADS * bq
    return _attention_call(_forward, bq, wide, t, [jax.ShapeDtypeStruct(q.shape, LOW), jax.ShapeDtypeStruct((HEADS, t), f32)],
                           [pltpu.VMEM((1, cols), f32), pltpu.VMEM((HEAD + 8, cols), f32), pltpu.VMEM((BK, cols), jnp.int32)], 4, [q, k, v])


def attend_bwd(q, k, v, do, lse, delta, bq=256, wide=256):
    t, f32, cols = q.shape[1], jnp.float32, HEADS * bq
    return _attention_call(_backward, bq, wide, t, [jax.ShapeDtypeStruct(a.shape, LOW) for a in (q, k, v)],
                           [pltpu.VMEM((HEAD, cols), f32), pltpu.VMEM((t, HEAD), f32), pltpu.VMEM((t, HEAD), f32), pltpu.VMEM((BK, cols), jnp.int32)],
                           10, [q, k, v, do, lse, delta])


from jax.sharding import PartitionSpec as P

THETA = 10000
NAMES = ("wq", "wk", "wv", "wo", "w_gate", "w_up", "w_down")
BT = 512
CF = 512
ONCE = pl.Buffered(1)


def _rms(h):
    wide = h.astype(jnp.float32)
    scale = lax.rsqrt(jnp.mean(wide * wide, -1, keepdims=True) + 1e-6)
    return wide, scale


def _low(x):
    return x.astype(jnp.bfloat16)


def _wide(x):
    return x.astype(jnp.float32)


def _swap_tiles(src, dst):
    r = src.shape[0] // 16
    for m in range(8):
        for n in range(8):
            t = _wide(src[2 * r * m : 2 * r * (m + 1), 256 * n : 256 * (n + 1)])
            top = jnp.concatenate([t[:r, :128], t[r:, :128]], axis=1)
            low = jnp.concatenate([t[:r, 128:], t[r:, 128:]], axis=1)
            dst[2 * r * n : 2 * r * (n + 1), 256 * m : 256 * (m + 1)] = jnp.concatenate([top, low], axis=0).astype(dst.dtype)


def _project(h_ref, cos_ref, sin_ref, *refs):
    *w_refs, q_ref, k_ref, v_ref = refs
    wide, scale = _rms(h_ref[...])
    a = _low(wide * scale)
    got = jnp.concatenate([_wide(_low(_dot(a, w[...], 1, 0))) for w in w_refs], axis=1)
    cos, sin = cos_ref[...], sin_ref[...]
    for i in range(6):
        t = got[:, 128 * i : 128 * (i + 1)]
        t = _low(t * cos + pltpu.roll(t, 64, 1) * sin)
        if i < 5:
            q_ref[i] = t
        else:
            k_ref[...] = t
    v_ref[...] = _low(got[:, 768:896])


def _out(wa_ref):
    return wa_ref[:, wa_ref.shape[1] - HEADS * HEAD :]


def _heads(o_ref):
    return jnp.concatenate([o_ref[i] for i in range(o_ref.shape[0])], axis=1)


def _mlp(o_ref, h_ref, wg_ref, wu_ref, wd_ref, wa_ref, y_ref, wdt_s, b_s, sum_s):
    @pl.when(pl.program_id(0) == 0)
    def _():
        _swap_tiles(wd_ref, wdt_s)

    mid = _low(_wide(h_ref[...]) + _wide(_low(_dot(_heads(o_ref), _out(wa_ref), 1, 0))))
    wide, scale = _rms(mid)
    b_s[...] = _low(wide * scale)
    sum_s[...] = jnp.zeros_like(sum_s)

    def chunk(c, _):
        at = pl.ds(pl.multiple_of(c * 2 * CF, 2 * CF), 2 * CF)
        gate, up = _dot(b_s[...], wg_ref[:, at], 1, 0), _dot(b_s[...], wu_ref[:, at], 1, 0)
        act = _low(gate * (1 / (1 + jnp.exp(-gate))) * up)
        sum_s[...] += _dot(act, wdt_s[:, at], 1, 1)

    lax.fori_loop(0, wg_ref.shape[1] // (2 * CF), chunk, None)
    y_ref[...] = _low(wide + _wide(_low(sum_s[...])))


def _mlp_back(*refs, joined):
    o_ref, h_ref, dy_ref, wg_ref, wu_ref, wd_ref, wa_ref = refs[:7]
    dh_ref, do_ref, delta_ref, g_ref, dwo_ref = refs[7 + joined : 12 + joined]
    wdt_s, ag_s, au_s, ad_s, ao_s, b_s, bt_s, dyt_s, db_s = refs[12 + joined :]
    step = pl.program_id(0)

    @pl.when(step == 0)
    def _():
        _swap_tiles(wd_ref, wdt_s)
        for s in (ag_s, au_s, ad_s, ao_s):
            s[...] = jnp.zeros_like(s)

    o = _heads(o_ref)
    mid = _low(_wide(h_ref[...]) + _wide(_low(_dot(o, _out(wa_ref), 1, 0))))
    wide, scale = _rms(mid)
    b = _low(wide * scale)
    b_s[...] = b
    bt_s[...] = b.T
    dyt_s[...] = dy_ref[...].T
    db_s[...] = jnp.zeros_like(db_s)

    def chunk(c):
        at = pl.ds(c * CF, CF)
        gate, up = _dot(b_s[...], wg_ref[:, at], 1, 0), _dot(b_s[...], wu_ref[:, at], 1, 0)
        dact = _wide(_low(_dot(dy_ref[...], wdt_s[:, at], 1, 0)))
        s = 1 / (1 + jnp.exp(-gate))
        silu = gate * s
        act = _low(silu * up)
        dup = _low(dact * silu)
        dgate = _low(dact * up * (s + silu * (1 - s)))
        ad_s[:, at] += _dot(dyt_s[...], act, 1, 0)
        au_s[:, at] += _dot(bt_s[...], dup, 1, 0)
        ag_s[:, at] += _dot(bt_s[...], dgate, 1, 0)
        db_s[...] += _dot(dup, wu_ref[:, at], 1, 1) + _dot(dgate, wg_ref[:, at], 1, 1)

    for c in range(wg_ref.shape[1] // CF):
        chunk(c)
    db = _wide(_low(db_s[...]))
    wide, scale = _rms(_low(_wide(h_ref[...]) + _wide(_low(_dot(o, _out(wa_ref), 1, 0)))))
    dn = scale * (db - wide * (scale * scale * jnp.mean(db * wide, -1, keepdims=True)))
    dh = _low(_wide(dy_ref[...]) + _wide(_low(dn)))
    dh_ref[...] = dh
    do = _low(_dot(dh, _out(wa_ref), 1, 1))
    for i in range(5):
        part = do[:, 128 * i : 128 * (i + 1)]
        do_ref[i] = part
        delta_ref[i : i + 1, :] = (_wide(part) * _wide(o_ref[i])).T.sum(axis=0, keepdims=True)
    ao_s[...] += _dot(o.T, dh, 1, 0)

    @pl.when(step == pl.num_programs(0) - 1)
    def _():
        ff = wg_ref.shape[1]
        g_ref[:, :ff] = _low(ag_s[...])
        g_ref[:, ff : 2 * ff] = _low(au_s[...])
        _swap_tiles(ad_s, g_ref.at[:, 2 * ff : 3 * ff])
        if joined:
            g_ref[:, 3 * ff :] = refs[7][...]
        dwo_ref[...] = _low(ao_s[...])


def _project_back(*refs, last):
    dq_ref, dk_ref, dv_ref, h_ref, cos_ref, sin_ref, dwo_ref = refs[:7]
    if last:
        g_ref, sum_s = refs[7:]
    else:
        wa_ref, dm_ref, dh_ref, g_ref, sum_s = refs[7:]
    step = pl.program_id(0)

    @pl.when(step == 0)
    def _():
        sum_s[...] = jnp.zeros_like(sum_s)

    cos, sin = cos_ref[...], sin_ref[...]
    parts = []
    for i in range(6):
        t = _wide(dq_ref[i] if i < 5 else dk_ref[...])
        parts.append(_low(t * cos - pltpu.roll(t, 64, 1) * sin))
    dqkv = jnp.concatenate(parts + [dv_ref[...]], axis=1)
    wide, scale = _rms(h_ref[...])
    sum_s[...] += _dot(_low(wide * scale).T, dqkv, 1, 0)
    if not last:
        da = _wide(_low(_dot(dqkv, wa_ref[:, :896], 1, 1)))
        dn = scale * (da - wide * (scale * scale * jnp.mean(da * wide, -1, keepdims=True)))
        dh_ref[...] = _low(_wide(dm_ref[...]) + _wide(_low(dn)))

    @pl.when(step == pl.num_programs(0) - 1)
    def _():
        g_ref[:, :896] = _low(sum_s[...])
        g_ref[:, 896:] = dwo_ref[...]


def _call(body, grid, ins, outs, scratch, flops, args, semantics="arbitrary"):
    size = sum(a.size * a.dtype.itemsize for a in args)
    return pl.pallas_call(
        body, grid=(grid,), in_specs=[s for s in ins], out_specs=[s for s, _ in outs], out_shape=[t for _, t in outs], scratch_shapes=scratch,
        compiler_params=pltpu.CompilerParams(dimension_semantics=(semantics,), vmem_limit_bytes=63 * 2**20),
        cost_estimate=pl.CostEstimate(flops=flops, transcendentals=0, bytes_accessed=size))(*args)


def _sizes(h):
    t, d = h.shape
    rows = pl.BlockSpec((BT, d), lambda i: (i, 0))
    heads = pl.BlockSpec((5, BT, HEAD), lambda i: (0, i, 0))
    head = pl.BlockSpec((BT, HEAD), lambda i: (i, 0))
    return t, d, rows, heads, head


def _part(d, ff, n, at):
    if n == 3:
        return pl.BlockSpec((d, 1536), lambda i: (0, 8), pipeline_mode=ONCE) if at else pl.BlockSpec((d, d), lambda i: (0, 22), pipeline_mode=ONCE)
    return pl.BlockSpec((d, ff), lambda i: (0, 3 * at + n), pipeline_mode=ONCE)


def _shape(s, t=jnp.bfloat16):
    return jax.ShapeDtypeStruct(s, t)


def project(h, cos, sin, *ws):
    t, d, rows, heads, head = _sizes(h)
    return _call(_project, t // BT, [rows, head, head] + [pl.BlockSpec((d, w.shape[1]), lambda i: (0, 0), pipeline_mode=ONCE) for w in ws],
                 [(heads, _shape((5, t, HEAD))), (head, _shape((t, HEAD))), (head, _shape((t, HEAD)))], [],
                 2 * t * d * 896, [h, cos, sin, *ws])


def mlp(o, h, slab, at):
    t, d, rows, heads, head = _sizes(h)
    ff = 2048
    return _call(_mlp, t // BT, [heads, rows] + [_part(d, ff, n, at) for n in range(4)], [(rows, _shape((t, d)))],
                 [pltpu.VMEM((d, ff), jnp.bfloat16), pltpu.VMEM((BT, d), jnp.bfloat16), pltpu.VMEM((BT, d), jnp.float32)],
                 2 * t * d * (d + 3 * ff), [o, h, slab, slab, slab, slab])[0]


def mlp_back(o, h, dy, slab, at, more=()):
    t, d, rows, heads, head = _sizes(h)
    ff = 2048
    whole = lambda s: pl.BlockSpec(s, lambda i: (0, 0), pipeline_mode=ONCE)
    wide = 3 * ff + sum(a.shape[1] for a in more)
    f32, b16 = jnp.float32, jnp.bfloat16
    return _call(functools.partial(_mlp_back, joined=len(more)), t // BT,
                 [heads, rows, rows] + [_part(d, ff, n, at) for n in range(4)] + [whole(a.shape) for a in more],
                 [(rows, _shape((t, d))), (heads, _shape((5, t, HEAD))), (pl.BlockSpec((5, BT), lambda i: (0, i)), _shape((5, t), f32)),
                  (whole((d, wide)), _shape((d, wide))), (whole((d, d)), _shape((d, d)))],
                 [pltpu.VMEM((d, ff), b16), pltpu.VMEM((d, ff), f32), pltpu.VMEM((d, ff), f32), pltpu.VMEM((d, ff), f32), pltpu.VMEM((d, d), f32),
                  pltpu.VMEM((BT, d), b16), pltpu.VMEM((d, BT), b16), pltpu.VMEM((d, BT), b16), pltpu.VMEM((BT, d), f32)],
                 2 * t * d * (3 * d + 8 * ff), [o, h, dy, slab, slab, slab, slab, *more])


def project_back(dq, dk, dv, h, cos, sin, dwo, slab=None, dm=None):
    t, d, rows, heads, head = _sizes(h)
    whole = lambda s: pl.BlockSpec(s, lambda i: (0, 0), pipeline_mode=ONCE)
    last = dm is None
    return _call(functools.partial(_project_back, last=last), t // BT,
                 [heads, head, head, rows, head, head, whole((d, d))] + ([] if last else [_part(d, 2048, 3, 1), rows]),
                 ([] if last else [(rows, _shape((t, d)))]) + [(whole((d, 1536)), _shape((d, 1536)))], [pltpu.VMEM((d, 896), jnp.float32)],
                 (2 if last else 4) * t * d * 896, [dq, dk, dv, h, cos, sin, dwo] + ([] if last else [slab, dm]))


def tables(t, theta):
    half = HEAD // 2
    angle = jnp.arange(t, dtype=jnp.float32)[:, None] * theta ** (-jnp.arange(half, dtype=jnp.float32) / half)
    cos, sin = jnp.cos(angle), jnp.sin(angle)
    return jnp.concatenate([cos, cos], 1), jnp.concatenate([-sin, sin], 1)


def adamw(w, m, v, g):
    m = 0.9 * m + 0.1 * g
    v = 0.95 * v + 0.05 * g * g
    step = m * lax.rsqrt(v + 1e-8) + 0.1 * w
    return (w - 0.02 * step).astype(jnp.bfloat16), m, v


def clipped(gradients, sum_of_squares, count):
    factor = jnp.minimum(1.0, 0.5 * lax.rsqrt(sum_of_squares / count + 1e-30))
    return [g * factor for g in gradients]


def laid(w):
    n, d = w["w_down"].shape
    down = w["w_down"].T.reshape(d * n // (128 * 40), 40, 128).transpose(1, 0, 2).reshape(40, -1)
    return [w["w_gate"], w["w_up"], down], [w["wq"], w["wk"], w["wv"], w["wo"]]


def parted(mlp, attn):
    ff = mlp.shape[1] // 3
    down = mlp[:, 2 * ff :].reshape(40, -1, 128).transpose(1, 0, 2).reshape(-1, 128).T
    return [attn[:, :640], attn[:, 640:768], attn[:, 768:896], attn[:, 896:], mlp[:, :ff], mlp[:, ff : 2 * ff], down]


def _total(n, x_ref, sum_ref, got, send, recv):
    me = lax.axis_index("dp")
    barrier = pltpu.get_barrier_semaphore()
    for k in range(1, n):
        pl.semaphore_signal(barrier, inc=1, device_id={"dp": lax.rem(me + k, n)}, device_id_type=pl.DeviceIdType.MESH)
    pl.semaphore_wait(barrier, n - 1)
    copies = [
        pltpu.make_async_remote_copy(src_ref=x_ref, dst_ref=got.at[me], send_sem=send.at[k - 1], recv_sem=recv.at[k - 1],
                                     device_id={"dp": lax.rem(me + k, n)}, device_id_type=pl.DeviceIdType.MESH)
        for k in range(1, n)
    ]
    for copy in copies:
        copy.start()
    got[me] = x_ref[...]
    for copy in copies:
        copy.wait()
    sum_ref[...] = functools.reduce(lambda a, b: a + b, [got[i] for i in range(n)])


def total(x, n):
    tile = (8, 128)
    vmem = pl.BlockSpec(memory_space=pltpu.VMEM)
    return pl.pallas_call(
        functools.partial(_total, n), out_shape=_shape(tile, jnp.float32), in_specs=[vmem], out_specs=vmem,
        scratch_shapes=[pltpu.VMEM((n, *tile), jnp.float32), pltpu.SemaphoreType.DMA((n - 1,)), pltpu.SemaphoreType.DMA((n - 1,))],
        compiler_params=pltpu.CompilerParams(collective_id=0, has_side_effects=True))(jnp.full(tile, x))[0, 0]


def solution(mesh):
    def scattered(g):
        return lax.psum_scatter(g, "dp", scatter_dimension=0, tiled=True)

    def exchanged(g):
        terms = lax.all_to_all(g.reshape(-1, 40, g.shape[1]), "dp", 0, 0, tiled=True)
        return lax.reduce_precision(_wide(terms).sum(0), 8, 7)

    def step(x, dy, *arrays):
        weights, m, v = (arrays[i : i + 7] for i in (0, 7, 14))
        x, dy = x[0], dy[0]
        def gathered(*parts):
            return lax.all_gather(jnp.concatenate(parts, 1), "dp", axis=0, tiled=True)

        mlps, attns = zip(*(laid({name: w[n] for name, w in zip(NAMES, weights)}) for n in range(2)))
        wq, wkv = gathered(attns[0][0]), gathered(*attns[0][1:3])
        slab = gathered(*mlps[0], *mlps[1], *attns[1], *attns[0][1:])
        cos, sin = tables(x.shape[0], THETA)

        q, k, v_ = project(x, cos, sin, wq, wkv)
        o, lse = attend(q, k, v_)
        h = mlp(o, x, slab, 0)
        kept = q, k, v_, o, lse
        q, k, v_ = project(h, cos, sin, slab[:, 12288:13184])
        o, lse = attend(q, k, v_)

        dm, do, delta, g, dwo = mlp_back(o, h, dy, slab, 1)
        first = scattered(g)
        dy, more = project_back(*attend_bwd(q, k, v_, do, lse, delta), h, cos, sin, dwo, slab, dm)
        fourth = scattered(more)
        q, k, v_, o, lse = kept
        dm, do, delta, g, dwo = mlp_back(o, x, dy, slab, 0)
        g, first = lax.optimization_barrier((g, first))
        second = scattered(g)
        g = project_back(*attend_bwd(q, k, v_, do, lse, delta), x, cos, sin, dwo)[0]
        third = exchanged(g)
        sums = first, second, third, fourth

        both = [parted(second, third), parted(first, fourth)]
        gradients = [jnp.stack([both[n][i] for n in range(2)]).astype(jnp.float32) for i in range(7)]
        squares = total(sum(jnp.sum(_wide(s) ** 2) for s in sums), mesh.shape["dp"])
        gradients = clipped(gradients, squares, lax.psum(1, "dp") * sum(g.size for g in gradients))
        new = [adamw(w.astype(jnp.float32), m, v, g) for w, m, v, g in zip(weights, m, v, gradients, strict=True)]
        return tuple(one[which] for which in range(3) for one in new)

    states, cut = P(("rep", "dp"), None, None), P(None, "dp", None)
    return jax.shard_map(
        step,
        mesh=mesh,
        in_specs=(states, states) + (cut,) * 21,
        out_specs=(P("rep", "dp", None),) * 21,
        check_vma=False,
    )
```
